32 devices in a mesh: grp: 2 (over x), seq: 8 (over z, y), head: 2 (over core).
Axes of the slice: x: 2, y: 2, z: 4, core: 2. Of those that a mesh axis runs over, the one named last changes fastest.
Arguments:
- patches: bfloat16 [3072, 1280], P(('grp', 'seq')), parts along dimension 0, may hold values from -6 to 6
- ln_gain: float32 [1280], replicated, may hold values from 0.25 to 1.75
- ln_bias: float32 [1280], replicated, may hold values from -3 to 3
- qkv_weight: bfloat16 [1280, 3, 1280], P(None, None, 'head'), may hold values from -0.15625 to 0.15625
- proj_weight: bfloat16 [1280, 1280], P('head'), may hold values from -0.15625 to 0.15625
- proj_bias: float32 [1280], replicated, may hold values from -3 to 3
- merge_gain: float32 [1280], replicated, may hold values from 0.25 to 1.75
- merge_bias: float32 [1280], replicated, may hold values from -3 to 3
- visual_kv_weight: bfloat16 [5120, 2, 512], P(None, None, 'head'), may hold values from -0.078125 to 0.078125
- image_tokens: int32 [32], P('grp'), parts along dimension 0, may hold values from 2 to 47, as said below
- text_before: int32 [32], P('grp'), parts along dimension 0, may hold values from 0 to 1024, as said below
- text_order: int32 [2048], P(('grp', 'seq')), parts along dimension 0, may hold values from 0 to 1023, each once
- queries: bfloat16 [2048, 4096], P(('grp', 'seq'), 'head'), parts along dimension 0, may hold values from -44 to 44
- text_kv: bfloat16 [2048, 2, 512], P(('grp', 'seq'), None, 'head'), parts along dimension 0, may hold values from -4 to 4
Outputs:
- attended: bfloat16 [2048, 4096], P(('grp', 'seq'), 'head'), parts along dimension 0
- visual_kv: bfloat16 [768, 2, 512], P(('grp', 'seq'), None, 'head'), parts along dimension 0
The draws below stay inside these ranges and needn't reach their ends.
There are 2 independent parts, one for each index of `grp`. The reference program is written for one: setup_inputs(seed, part) draws one part's arguments, and reference() takes and returns one part's arrays. A program takes and returns all parts, laid end to end along the dimension named above; an argument that names none is the same for every part. Nothing has to cross between parts.
Inputs may be any that keep to these rules, and one draw needn't show every extreme that they name: `image_tokens`: they sum to 384; each run of 48 visual tokens of one index of seq holds the last token of exactly two images (the last index: of one image and of the last image), so an image crosses every boundary between indices; the last image holds 47 tokens. `text_before`: non-decreasing. `text_order`: each number once.
All inputs are finite; a program needn't handle non-finite values.
Results may differ from the reference program's by a relative error of at most 0.0095.
Values may be sent and summed in bfloat16 or wider, within the bound.
No kernel may reach another device: no remote copies, remote signals or barrier semaphores. Data moves between devices by JAX's collectives and lax.ppermute only.
A program may use at most 128 MiB of HBM per device.

```python
import math
import jax
import jax.numpy as jnp
from jax import lax

VIT_D = 1280
VIT_HEADS = 16
VIT_HD = 80
HEAD_DIM = 128
GROUP = 8
KV_HEADS = 4
PATCH_DEV = 192
TOK_DEV = 128
VT_DEV = 48
MERGED = 5120
KVW = 512
QW = 4096
IMAGES = 16
PATCHES = 1536
VIS = 384
TOKENS = 1024
N_SEQ = 8


def shared_keys(key):
    drawn = jax.random.normal(jax.random.fold_in(key, 11), (TOKENS, KV_HEADS, HEAD_DIM), jnp.float32)
    return jnp.clip(drawn, -4.0, 4.0)


def draw_queries(key, part):
    drawn_draw = jax.random.normal(jax.random.fold_in(key, 12), (TOKENS, KV_HEADS, GROUP, HEAD_DIM), jnp.float32)
    drawn_draw = jnp.clip(drawn_draw, -4.0, 4.0)
    return drawn_draw.reshape(TOKENS, QW).astype(jnp.bfloat16)


def draw_text_kv(key, part):
    keys_drawn = shared_keys(key).reshape(TOKENS, KVW)
    values_drawn = jnp.clip(jax.random.normal(jax.random.fold_in(key, 14), (TOKENS, KVW), jnp.float32), -4.0, 4.0)
    return jnp.stack([keys_drawn, values_drawn], axis=1).astype(jnp.bfloat16)


def draw_text_before(key, part):
    drawn = jax.random.randint(jax.random.fold_in(key, 15), (IMAGES,), 0, TOKENS + 1)
    return jnp.sort(drawn).astype(jnp.int32)


def draw_image_tokens(key, part):
    quarter = VT_DEV // 4
    device_starts = jnp.arange(N_SEQ, dtype=jnp.int32) * VT_DEV
    early_cuts = jax.random.randint(jax.random.fold_in(key, 21), (N_SEQ,), 2, quarter + 2).astype(jnp.int32) + device_starts
    early_cuts = early_cuts.at[N_SEQ - 1].set((N_SEQ - 1) * VT_DEV + 1)
    late_cuts = jax.random.randint(jax.random.fold_in(key, 22), (N_SEQ - 1,), VT_DEV - quarter, VT_DEV).astype(jnp.int32) + device_starts[:-1]
    paired = jnp.stack([early_cuts[:-1], late_cuts], axis=1).reshape(2 * N_SEQ - 2)
    image_ends = jnp.concatenate([paired, early_cuts[N_SEQ - 1:], jnp.full((1,), VIS, jnp.int32)])
    image_starts = jnp.concatenate([jnp.zeros((1,), jnp.int32), image_ends[:-1]])
    return (image_ends - image_starts).astype(jnp.int32)


def steps_of(own_key, shape, pieces, least, top_value):
    level, own = 1.0, jax.random.fold_in(own_key, 6)
    for dim, blocks in pieces:
        draws = jnp.exp(jax.random.uniform(jax.random.fold_in(own, dim), (blocks,), jnp.float32, least / len(pieces), top_value / len(pieces)))
        level = level * jnp.repeat(draws, shape[dim] // blocks).reshape([-1 if axis == dim else 1 for axis in range(len(shape))])
    return level


def noise(stream_key, shape, scale, limit, split=(), kind=jnp.bfloat16):
    values = scale * jax.random.normal(stream_key, shape, jnp.float32)
    if split:
        values = values * steps_of(stream_key, shape, split, -0.22, 0.18)
    return jnp.clip(values, -limit, limit).astype(kind)


def setup_inputs(seed: int = 0, part: int = 0) -> dict:
    splits = jax.random.split(jax.random.key(seed), 15)
    own_keys = jax.random.split(jax.random.fold_in(splits[14], part), 15)
    patches = noise(own_keys[0], (PATCHES, VIT_D), 1.0, 6.0, ((0, 8),))
    ln_gain = jnp.clip(1.0 + 0.15 * jax.random.normal(splits[1], (VIT_D,), jnp.float32), 0.25, 1.75)
    ln_bias = noise(splits[2], (VIT_D,), 0.5, 3.0, (), jnp.float32)
    qkv_weight = noise(splits[3], (VIT_D, 3, VIT_D), VIT_D ** -0.5, 0.15625, ((2, 2),))
    proj_weight = noise(splits[4], (VIT_D, VIT_D), VIT_D ** -0.5, 0.15625, ((0, 2),))
    proj_bias = noise(splits[5], (VIT_D,), 0.5, 3.0, (), jnp.float32)
    merge_gain = jnp.clip(1.0 + 0.15 * jax.random.normal(splits[6], (VIT_D,), jnp.float32), 0.25, 1.75)
    merge_bias = noise(splits[7], (VIT_D,), 0.5, 3.0, (), jnp.float32)
    visual_kv_weight = noise(splits[8], (MERGED, 2, KVW), MERGED ** -0.5, 0.078125, ((2, 2),))
    image_tokens = draw_image_tokens(jax.random.fold_in(jax.random.fold_in(splits[14], part), 71), part)
    text_before = draw_text_before(jax.random.fold_in(jax.random.fold_in(splits[14], part), 71), part)
    text_order = jax.random.permutation(own_keys[11], TOKENS).astype(jnp.int32)
    queries = draw_queries(jax.random.fold_in(jax.random.fold_in(splits[14], part), 71), part)
    text_kv = draw_text_kv(jax.random.fold_in(jax.random.fold_in(splits[14], part), 71), part)
    return dict(patches=patches, ln_gain=ln_gain, ln_bias=ln_bias, qkv_weight=qkv_weight, proj_weight=proj_weight, proj_bias=proj_bias, merge_gain=merge_gain, merge_bias=merge_bias, visual_kv_weight=visual_kv_weight, image_tokens=image_tokens, text_before=text_before, text_order=text_order, queries=queries, text_kv=text_kv)


epsilon = 1e-06
masked_score = -1e+30

def layer_norm(inputs, scale_gain, shift_bias):
    centre = lax.optimization_barrier(jnp.mean(inputs, axis=-1, keepdims=True))
    centred = inputs - centre
    spread = lax.optimization_barrier(jnp.mean(centred * centred, axis=-1, keepdims=True))
    return centred * lax.rsqrt(spread + epsilon) * scale_gain + shift_bias

def reference(patches, ln_gain, ln_bias, qkv_weight, proj_weight, proj_bias, merge_gain, merge_bias, visual_kv_weight, image_tokens, text_before, text_order, queries, text_kv):
    normed = layer_norm(patches.astype(jnp.float32), ln_gain, ln_bias).astype(jnp.bfloat16)
    projected = jnp.dot(normed, qkv_weight.reshape(VIT_D, 3 * VIT_D), preferred_element_type=jnp.float32).astype(jnp.bfloat16)
    projected = projected.reshape(PATCHES, 3, VIT_HEADS, VIT_HD)
    image_ends = 4 * jnp.cumsum(image_tokens)
    patch_index = jnp.arange(PATCHES, dtype=jnp.int32)
    image_id = lax.optimization_barrier(jnp.sum((patch_index[:, None] >= image_ends[None, :]).astype(jnp.int32), axis=1))
    padded_kv = jnp.pad(projected[:, 1:], ((PATCH_DEV, PATCH_DEV), (0, 0), (0, 0), (0, 0)))
    padded_ids = jnp.pad(image_id, (PATCH_DEV, PATCH_DEV), constant_values=-1)

    def vit_block(block_index):
        first_row = block_index * PATCH_DEV
        block_query = lax.dynamic_slice_in_dim(projected[:, 0], first_row, PATCH_DEV, 0).astype(jnp.float32)
        block_kv = lax.dynamic_slice_in_dim(padded_kv, first_row, 3 * PATCH_DEV, 0).astype(jnp.float32)
        query_ids = lax.dynamic_slice_in_dim(image_id, first_row, PATCH_DEV, 0)
        key_ids = lax.dynamic_slice_in_dim(padded_ids, first_row, 3 * PATCH_DEV, 0)
        scores = jnp.einsum('qhd,khd->hqk', block_query, block_kv[:, 0]) / math.sqrt(VIT_HD)
        allowed = query_ids[:, None] == key_ids[None, :]
        scores = jnp.where(allowed[None], scores, masked_score)
        weights = jax.nn.softmax(scores, axis=-1)
        rounded = lax.optimization_barrier(weights.astype(jnp.bfloat16)).astype(jnp.float32)
        mixed_rows = jnp.einsum('hqk,khd->qhd', rounded, block_kv[:, 1])
        return mixed_rows.astype(jnp.bfloat16).reshape(PATCH_DEV, VIT_D)
    vit_mixed = lax.map(vit_block, jnp.arange(N_SEQ, dtype=jnp.int32)).reshape(PATCHES, VIT_D)
    encoded = patches.astype(jnp.float32) + jnp.dot(vit_mixed, proj_weight, preferred_element_type=jnp.float32) + proj_bias
    encoded = encoded.astype(jnp.bfloat16)
    merged = layer_norm(encoded.astype(jnp.float32), merge_gain, merge_bias).astype(jnp.bfloat16).reshape(VIS, MERGED)
    visual_kv = jnp.dot(merged, visual_kv_weight.reshape(MERGED, 2 * KVW), preferred_element_type=jnp.float32)
    visual_kv = visual_kv.astype(jnp.bfloat16).reshape(VIS, 2, KVW)
    text_pos = text_order + lax.optimization_barrier(jnp.sum(jnp.where(text_before[None, :] <= text_order[:, None], image_tokens[None, :], 0), axis=1))
    image_starts = jnp.cumsum(image_tokens) - image_tokens
    steps_before = text_before - jnp.concatenate([jnp.zeros((1,), jnp.int32), text_before[:-1]])
    visual_index = jnp.arange(VIS, dtype=jnp.int32)
    vis_pos = visual_index + lax.optimization_barrier(jnp.sum(jnp.where(image_starts[None, :] <= visual_index[:, None], steps_before[None, :], 0), axis=1))
    all_kv = jnp.concatenate([text_kv, visual_kv], axis=0)
    all_pos = jnp.concatenate([text_pos, vis_pos])

    def llm_block(block_index):
        row_block = block_index // KV_HEADS
        kv_head = block_index % KV_HEADS
        block_query = lax.dynamic_slice_in_dim(queries, row_block * TOK_DEV, TOK_DEV, 0)
        block_query = lax.dynamic_slice_in_dim(block_query, kv_head * GROUP * HEAD_DIM, GROUP * HEAD_DIM, 1)
        block_query = block_query.astype(jnp.float32).reshape(TOK_DEV, GROUP, HEAD_DIM)
        query_pos = lax.dynamic_slice_in_dim(text_pos, row_block * TOK_DEV, TOK_DEV, 0)
        head_keys = lax.dynamic_slice_in_dim(all_kv[:, 0], kv_head * HEAD_DIM, HEAD_DIM, 1).astype(jnp.float32)
        head_values = lax.dynamic_slice_in_dim(all_kv[:, 1], kv_head * HEAD_DIM, HEAD_DIM, 1).astype(jnp.float32)
        scores = jnp.einsum('qgd,kd->qgk', block_query, head_keys) / math.sqrt(HEAD_DIM)
        allowed = (all_pos[None, :] <= query_pos[:, None])[:, None, :]
        scores = jnp.where(allowed, scores, masked_score)
        row_max = lax.optimization_barrier(jnp.max(scores, axis=-1, keepdims=True))
        weights = jnp.where(allowed, jnp.exp(scores - row_max), 0.0)
        row_sum = lax.optimization_barrier(jnp.sum(weights, axis=-1))
        rounded = lax.optimization_barrier(weights.astype(jnp.bfloat16)).astype(jnp.float32)
        summed = jnp.einsum('qgk,kd->qgd', rounded, head_values)
        return (summed / row_sum[..., None]).reshape(TOK_DEV, GROUP * HEAD_DIM)
    outputs = lax.map(llm_block, jnp.arange(N_SEQ * KV_HEADS, dtype=jnp.int32))
    outputs = outputs.reshape(N_SEQ, KV_HEADS, TOK_DEV, GROUP * HEAD_DIM)
    attended = jnp.transpose(outputs, (0, 2, 1, 3)).reshape(TOKENS, QW)
    return (attended.astype(jnp.bfloat16), visual_kv)
```

```python
import functools
import math

import jax
import jax.numpy as jnp
from jax import lax
from jax.experimental import pallas as pl
from jax.experimental.pallas import tpu as pltpu
from jax.sharding import PartitionSpec as P

VIT_HD = 80
HEAD_DIM = 128
GROUP = 8
LANES = 128

epsilon = 1e-06
masked_score = -1e30


f32 = jnp.float32
bf16 = jnp.bfloat16


def layer_norm(inputs, scale_gain, shift_bias):
    centre = jnp.mean(inputs, axis=-1, keepdims=True)
    centred = inputs - centre
    spread = jnp.mean(centred * centred, axis=-1, keepdims=True)
    return centred * lax.rsqrt(spread + epsilon) * scale_gain + shift_bias


def vmem_call(body, out_shape, scratch=(), flops=0, nbytes=0, trans=0, name=None):
    spec = pl.BlockSpec(memory_space=pltpu.VMEM)

    def run(*args):
        multi = isinstance(out_shape, (tuple, list))
        return pl.pallas_call(
            body,
            out_shape=out_shape,
            in_specs=[spec] * len(args),
            out_specs=[spec] * len(out_shape) if multi else spec,
            scratch_shapes=scratch,
            cost_estimate=pl.CostEstimate(flops=flops, bytes_accessed=nbytes, transcendentals=trans),
            name=name,
        )(*args)

    return run


def project_kernel(first, rows_ref, gain_ref, bias_ref, weight_ref, *out_refs):
    normed = layer_norm(rows_ref[...].astype(f32), gain_ref[...], bias_ref[...]).astype(bf16)
    for j, out_ref in enumerate(out_refs):
        out_ref[...] = jnp.dot(normed, weight_ref[first + j], preferred_element_type=f32).astype(bf16)


def project(rows, gain, bias, weight, first, name):
    count = 3 - first
    out = jax.ShapeDtypeStruct((rows.shape[0], weight.shape[2]), bf16)
    return vmem_call(
        functools.partial(project_kernel, first),
        (out,) * count,
        flops=2 * rows.shape[0] * weight.shape[1] * weight.shape[2] * count,
        nbytes=weight.size * 2,
        name=name,
    )(rows, gain, bias, weight)


def vit_kernel(parts, own_ids_ref, near_ids_ref, proj_ref, q_ref, *refs):
    key_refs, value_refs = refs[:parts], refs[parts : 2 * parts]
    out_ref, keys, values, mixed = refs[2 * parts :]
    row = 0
    for key_ref, value_ref in zip(key_refs, value_refs):
        n = key_ref.shape[0]
        keys[row : row + n, :] = key_ref[...]
        values[row : row + n, :] = value_ref[...]
        row += n
    allowed = own_ids_ref[...] == near_ids_ref[...]
    head_cols = q_ref.shape[1]
    factor = math.log2(math.e) / math.sqrt(VIT_HD)
    for h in range(head_cols // VIT_HD):
        first, last = h * VIT_HD, (h + 1) * VIT_HD
        low, high = first // LANES * LANES, -(-last // LANES) * LANES
        column = low + lax.broadcasted_iota(jnp.int32, (1, high - low), 1)
        inside = (column >= first) & (column < last)
        query = jnp.where(inside, q_ref[:, low:high], jnp.zeros((), bf16))
        scores = lax.dot_general(
            query, keys[:, low:high], (((1,), (1,)), ((), ())), preferred_element_type=f32
        )
        scores = jnp.where(allowed, scores * factor, masked_score)
        weights = jnp.exp2(scores - jnp.max(scores, axis=1, keepdims=True))
        total = jnp.sum(weights, axis=1, keepdims=True)
        part = jnp.dot(weights.astype(bf16), values[:, low:high], preferred_element_type=f32)
        part = (part / total).astype(bf16)
        if first == low:
            mixed[:, low:high] = part
        else:
            split = low + LANES
            mixed[:, low:split] = jnp.where(inside[:, :LANES], part[:, :LANES], mixed[:, low:split])
            if high > split:
                mixed[:, split:high] = part[:, LANES:]
    out_ref[...] = jnp.dot(mixed[...], proj_ref[...], preferred_element_type=f32).astype(bf16)


def merge_kernel(rows_ref, mine_ref, other_ref, pbias_ref, gain_ref, bias_ref, weight_ref, out_ref, merged):
    encoded = rows_ref[...].astype(f32) + (mine_ref[...].astype(f32) + other_ref[...].astype(f32)) + pbias_ref[...]
    encoded = encoded.astype(bf16).astype(f32)
    normed = layer_norm(encoded, gain_ref[...], bias_ref[...])
    rows, width = normed.shape
    for c in range(width // LANES):
        merged[c * rows : (c + 1) * rows, :] = normed[:, c * LANES : (c + 1) * LANES]
    total = None
    for i in range(4):
        piece = jnp.concatenate(
            [merged[pl.ds(c * rows + i, rows // 4, stride=4), :] for c in range(width // LANES)], axis=1
        ).astype(bf16)
        term = jnp.dot(piece, weight_ref[i * width : (i + 1) * width, :], preferred_element_type=f32)
        total = term if total is None else total + term
    out_ref[...] = total.astype(bf16)


def block_scores(q_ref, kv, pos, query_pos, consume):
    tokens = q_ref.shape[0]
    heads = kv.shape[1] // (2 * HEAD_DIM)
    factor = math.log2(math.e) / math.sqrt(HEAD_DIM)
    visible = pos <= query_pos
    for h in range(heads):
        keys = kv[:, h * HEAD_DIM : (h + 1) * HEAD_DIM]
        values = kv[:, (heads + h) * HEAD_DIM : (heads + h + 1) * HEAD_DIM]
        for g in range(GROUP):
            j = h * GROUP + g
            query = q_ref[:, j * HEAD_DIM : (j + 1) * HEAD_DIM]
            scores = lax.dot_general(query, keys, (((1,), (1,)), ((), ())), preferred_element_type=f32)
            scores = jnp.where(visible, scores * factor, masked_score)
            top = jnp.max(scores, axis=1, keepdims=True)
            weights = jnp.exp2(scores - top)
            total = jnp.sum(weights, axis=1, keepdims=True)
            part = jnp.dot(weights.astype(bf16), values, preferred_element_type=f32)
            consume(j, top, total, part)


def text_kernel(tokens, query_pos_ref, q_ref, block_ref, out_ref, top_ref, sum_ref, kv, pos):
    rows = block_ref.shape[0]
    stride = tokens + 8
    for b in range(rows // stride):
        kv[b * tokens : (b + 1) * tokens, :] = block_ref[b * stride : b * stride + tokens, :]
        tail = block_ref[b * stride + tokens : (b + 1) * stride, :tokens].astype(f32)
        pos[:, b * tokens : (b + 1) * tokens] = tail[0:1, :] * 128.0 + tail[1:2, :]
    lane = lax.broadcasted_iota(jnp.int32, top_ref.shape, 1)

    def consume(j, top, total, part):
        out_ref[:, j * HEAD_DIM : (j + 1) * HEAD_DIM] = part
        if j == 0:
            top_ref[...] = jnp.broadcast_to(top, top_ref.shape)
            sum_ref[...] = jnp.broadcast_to(total, sum_ref.shape)
        else:
            top_ref[...] = jnp.where(lane == j, top, top_ref[...])
            sum_ref[...] = jnp.where(lane == j, total, sum_ref[...])

    block_scores(q_ref, kv, pos[...], query_pos_ref[...], consume)


def text_part(query_pos, queries, block, tokens, name):
    rows = queries.shape[0]
    count = block.shape[0] // (tokens + 8) * tokens
    heads = queries.shape[1] // HEAD_DIM
    return vmem_call(
        functools.partial(text_kernel, tokens),
        (
            jax.ShapeDtypeStruct(queries.shape, f32),
            jax.ShapeDtypeStruct((rows, LANES), f32),
            jax.ShapeDtypeStruct((rows, LANES), f32),
        ),
        scratch=(pltpu.VMEM((count, block.shape[1]), bf16), pltpu.VMEM((1, count), f32)),
        flops=4 * rows * queries.shape[1] * count,
        nbytes=2 * (queries.size + block.size) + 4 * queries.size,
        trans=rows * heads * count,
        name=name,
    )(query_pos, queries, block)


def last_kernel(parts, blocks, query_pos_ref, q_ref, pos_ref, *refs):
    block_refs, refs = refs[:blocks], refs[blocks:]
    part_refs, (out_ref, kv) = refs[: 3 * parts], refs[3 * parts :]
    row = 0
    for block_ref in block_refs:
        kv[row : row + block_ref.shape[0], :] = block_ref[...]
        row += block_ref.shape[0]
    earlier = [part_refs[3 * i : 3 * i + 3] for i in range(parts)]

    def consume(j, top, total, part):
        columns = slice(j * HEAD_DIM, (j + 1) * HEAD_DIM)
        tops = [t[:, j : j + 1] for _, t, _ in earlier]
        best = top
        for t in tops:
            best = jnp.maximum(best, t)
        scale = jnp.exp2(top - best)
        numer, denom = part * scale, total * scale
        for (o, _, s), t in zip(earlier, tops):
            scale = jnp.exp2(t - best)
            numer = numer + o[:, columns] * scale
            denom = denom + s[:, j : j + 1] * scale
        out_ref[:, columns] = (numer / denom).astype(bf16)

    block_scores(q_ref, kv, pos_ref[...], query_pos_ref[...], consume)


def last_part(query_pos, queries, pos, blocks, parts):
    rows = queries.shape[0]
    count = pos.shape[1]
    heads = queries.shape[1] // HEAD_DIM
    return vmem_call(
        functools.partial(last_kernel, len(parts), len(blocks)),
        jax.ShapeDtypeStruct(queries.shape, bf16),
        scratch=(pltpu.VMEM((count, blocks[0].shape[1]), bf16),),
        flops=4 * rows * queries.shape[1] * count,
        nbytes=4 * queries.size * (len(parts) + 1),
        trans=rows * heads * count,
        name="last_part",
    )(query_pos, queries, pos, *blocks, *[a for part in parts for a in part])


def vis_kernel(tokens, query_pos_ref, q_ref, pos_ref, block_ref, out_ref, top_ref, sum_ref):
    lane = lax.broadcasted_iota(jnp.int32, top_ref.shape, 1)
    top_ref[...] = jnp.zeros_like(top_ref)
    sum_ref[...] = jnp.zeros_like(sum_ref)

    def consume(j, top, total, part):
        out_ref[:, j * HEAD_DIM : (j + 1) * HEAD_DIM] = part
        top_ref[...] = jnp.where(lane == j, top, top_ref[...])
        sum_ref[...] = jnp.where(lane == j, total, sum_ref[...])

    block_scores(q_ref, block_ref, pos_ref[...], query_pos_ref[...], consume)


def vis_part(query_pos, queries, pos, block):
    rows = queries.shape[0]
    return vmem_call(
        functools.partial(vis_kernel, 0),
        (
            jax.ShapeDtypeStruct(queries.shape, f32),
            jax.ShapeDtypeStruct((rows, LANES), f32),
            jax.ShapeDtypeStruct((rows, LANES), f32),
        ),
        flops=4 * rows * queries.shape[1] * block.shape[0],
        nbytes=4 * queries.size,
        name="vis_part",
    )(query_pos, queries, pos, block)


def per_device(
    patches,
    ln_gain,
    ln_bias,
    qkv_weight,
    proj_weight,
    proj_bias,
    merge_gain,
    merge_bias,
    visual_kv_weight,
    image_tokens,
    text_before,
    text_order,
    queries,
    text_kv,
):
    seq_index = lax.axis_index("seq")
    seq_count = lax.axis_size("seq")
    head_index = lax.axis_index("head")
    head_count = lax.axis_size("head")
    patch_rows, model_width = patches.shape
    merged_rows = patch_rows // 4
    head_cols = qkv_weight.shape[2]
    tokens = queries.shape[0]
    kv_width = text_kv.shape[1] * text_kv.shape[2]
    small = seq_count == 8 and head_count == 2
    ahead = [(i, i + 1) for i in range(seq_count - 1)]
    back = [(i + 1, i) for i in range(seq_count - 1)]

    if head_count == 2:
        half = patch_rows // 2
        mine = lax.dynamic_slice_in_dim(patches, head_index * half, half, 0)
    else:
        half = patch_rows
        mine = patches
    before_mine = lax.ppermute(mine, "seq", ahead)
    after_mine = lax.ppermute(mine, "seq", back)

    text_pos = text_order + jnp.sum(
        jnp.where(text_before[None, :] <= text_order[:, None], image_tokens[None, :], 0), axis=1
    )
    digits = jnp.stack([text_pos // 128, text_pos % 128]).astype(bf16)
    digits = jnp.pad(digits, ((0, 6), (0, kv_width - tokens)))
    block = jnp.concatenate([text_kv.reshape(tokens, kv_width), digits], axis=0)
    if small:
        column = [block] + [
            lax.ppermute(block, "seq", [(i, (i + 2 * k) % 8) for i in range(8)]) for k in (1, 2, 3)
        ]
        column = jnp.concatenate(column, axis=0)
        text_blocks = [column, lax.ppermute(column, "seq", [(i, i ^ 1) for i in range(8)])]
    else:
        gathered = lax.all_gather(block, "seq", axis=0, tiled=True)
        step = 8 * (tokens + 8)
        text_blocks = [gathered[i : i + step] for i in range(0, gathered.shape[0], step)]

    weight = jnp.transpose(qkv_weight, (1, 0, 2))
    gain, bias = ln_gain[None, :], ln_bias[None, :]
    query, key_own, value_own = project(patches, gain, bias, weight, 0, "own_qkv")

    key_parts, value_parts, starts = [key_own], [value_own], [(0, patch_rows)]
    shift = head_index * half if head_count == 2 else 0
    neighbours = [(before_mine, shift - patch_rows), (after_mine, shift + patch_rows)]
    if head_count == 2:
        swap = [(0, 1), (1, 0)]
        other = half - shift
        neighbours += [
            (lax.ppermute(before_mine, "head", swap), other - patch_rows),
            (lax.ppermute(after_mine, "head", swap), other + patch_rows),
        ]
    for rows, start in neighbours:
        k, v = project(rows, gain, bias, weight, 1, "near_kv")
        key_parts.append(k)
        value_parts.append(v)
        starts.append((start, half))
    image_ends = 4 * jnp.cumsum(image_tokens)
    near_index = seq_index * patch_rows + jnp.concatenate(
        [start + jnp.arange(n, dtype=jnp.int32) for start, n in starts]
    )
    near_ids = jnp.sum((near_index[:, None] >= image_ends[None, :]).astype(jnp.int32), axis=1)
    near_ids = jnp.where((near_index >= 0) & (near_index < patch_rows * seq_count), near_ids, -1)
    near_count = near_index.shape[0]
    mine_part = vmem_call(
        functools.partial(vit_kernel, len(key_parts)),
        jax.ShapeDtypeStruct((patch_rows, model_width), bf16),
        scratch=(
            pltpu.VMEM((near_count, head_cols), bf16),
            pltpu.VMEM((near_count, head_cols), bf16),
            pltpu.VMEM((patch_rows, head_cols), bf16),
        ),
        flops=4 * patch_rows * near_count * head_cols + 2 * patch_rows * head_cols * model_width,
        nbytes=2 * proj_weight.size,
        trans=patch_rows * near_count * head_cols // VIT_HD,
        name="vit_attention",
    )(near_ids[:patch_rows, None], near_ids[None, :], proj_weight, query, *key_parts, *value_parts)
    if head_count == 2:
        other_part = lax.ppermute(mine_part, "head", [(0, 1), (1, 0)])
    else:
        other_part = lax.psum(mine_part, "head") - mine_part
    weight_kv = visual_kv_weight.reshape(4 * model_width, -1)
    visual = vmem_call(
        merge_kernel,
        jax.ShapeDtypeStruct((merged_rows, kv_width), bf16),
        scratch=(pltpu.VMEM((patch_rows * (model_width // LANES), LANES), f32),),
        flops=2 * merged_rows * weight_kv.size,
        nbytes=2 * weight_kv.size,
        name="merge",
    )(patches, mine_part, other_part, proj_bias[None, :], merge_gain[None, :], merge_bias[None, :], weight_kv)

    if small:
        pair = jnp.concatenate([visual, lax.ppermute(visual, "seq", [(i, i ^ 1) for i in range(8)])])
        visual_blocks, sources = [pair], [seq_index, seq_index ^ 1]
        for k in (1, 2, 3):
            visual_blocks.append(lax.ppermute(pair, "seq", [(i, (i + 2 * k) % 8) for i in range(8)]))
            source = (seq_index - 2 * k) % 8
            sources += [source, source ^ 1]
        sources = jnp.stack(sources)
    else:
        gathered = lax.all_gather(visual, "seq", axis=0, tiled=True)
        sources = jnp.arange(seq_count, dtype=jnp.int32)
        step = 8 * merged_rows
        visual_blocks = [gathered[i : i + step] for i in range(0, gathered.shape[0], step)]
    image_starts = jnp.cumsum(image_tokens) - image_tokens
    steps_before = text_before - jnp.concatenate([jnp.zeros((1,), jnp.int32), text_before[:-1]])
    visual_index = (sources[:, None] * merged_rows + jnp.arange(merged_rows, dtype=jnp.int32)).reshape(-1)
    vis_pos = visual_index + jnp.sum(
        jnp.where(image_starts[None, :] <= visual_index[:, None], steps_before[None, :], 0), axis=1
    )
    vis_pos = vis_pos.astype(f32)[None, :]
    query_pos = text_pos.astype(f32)[:, None]

    parts = [
        text_part(query_pos, queries, text_block, tokens, "text_part") for text_block in text_blocks
    ]
    if not small:
        step = visual_blocks[0].shape[0]
        for i, visual_block in enumerate(visual_blocks[:-1]):
            parts.append(vis_part(query_pos, queries, vis_pos[:, i * step : (i + 1) * step], visual_block))
        vis_pos = vis_pos[:, (len(visual_blocks) - 1) * step :]
        visual_blocks = visual_blocks[-1:]
    attended = last_part(query_pos, queries, vis_pos, visual_blocks, parts)
    return (attended, visual.reshape(merged_rows, text_kv.shape[1], -1))


def solution(mesh):
    in_specs = (
        P(("grp", "seq"), None),
        P(),
        P(),
        P(None, None, "head"),
        P("head", None),
        P(),
        P(),
        P(),
        P(None, None, "head"),
        P("grp"),
        P("grp"),
        P(("grp", "seq")),
        P(("grp", "seq"), "head"),
        P(("grp", "seq"), None, "head"),
    )
    out_specs = (P(("grp", "seq"), "head"), P(("grp", "seq"), None, "head"))
    return jax.shard_map(
        per_device, mesh=mesh, in_specs=in_specs, out_specs=out_specs, check_vma=False
    )
```

```python
import functools
import math

import jax
import jax.numpy as jnp
from jax import lax
from jax.experimental import pallas as pl
from jax.experimental.pallas import tpu as pltpu
from jax.sharding import PartitionSpec as P

VIT_HD = 80
HEAD_DIM = 128
GROUP = 8
LANES = 128

epsilon = 1e-06
masked_score = -1e30


f32 = jnp.float32
bf16 = jnp.bfloat16


def layer_norm(inputs, scale_gain, shift_bias):
    centre = jnp.mean(inputs, axis=-1, keepdims=True)
    centred = inputs - centre
    spread = jnp.mean(centred * centred, axis=-1, keepdims=True)
    return centred * lax.rsqrt(spread + epsilon) * scale_gain + shift_bias


def padded_bytes(shape, dtype):
    item = jnp.dtype(dtype).itemsize
    rows = shape[-2] if len(shape) > 1 else 1
    count = math.prod(shape[:-2]) * (-(-rows // 16) * 16) * (-(-shape[-1] // LANES) * LANES)
    return count * item


def vmem_call(body, out_shape, scratch=(), flops=0, nbytes=0, trans=0, name=None, spaces=None, spare=6 << 20):
    spaces = spaces or {}

    def run(*args):
        multi = isinstance(out_shape, (tuple, list))
        outs = out_shape if multi else (out_shape,)
        held = [a for i, a in enumerate(args) if i not in spaces] + list(outs)
        held += [a for a in scratch if a.memory_space == pltpu.VMEM]
        size = sum(padded_bytes(a.shape, a.dtype) for a in held)
        spec = pl.BlockSpec(memory_space=pltpu.VMEM)
        return pl.pallas_call(
            body,
            out_shape=out_shape,
            in_specs=[pl.BlockSpec(memory_space=spaces.get(i, pltpu.VMEM)) for i in range(len(args))],
            out_specs=[spec] * len(out_shape) if multi else spec,
            scratch_shapes=scratch,
            compiler_params=pltpu.CompilerParams(vmem_limit_bytes=size + spare),
            cost_estimate=pl.CostEstimate(flops=flops, bytes_accessed=nbytes, transcendentals=trans),
            name=name,
        )(*args)

    return run


def layer_norm_rows(refs, gain_ref, bias_ref):
    width = gain_ref.shape[0]
    rows = jnp.concatenate([ref[...] for ref in refs], axis=0).astype(f32)
    return layer_norm(rows, gain_ref[...].reshape(1, width), bias_ref[...].reshape(1, width)).astype(bf16)


def pick(index, segments):
    out = index + segments[0][1]
    for offset, start in segments[1:]:
        out = jnp.where(index >= offset, index - offset + start, out)
    return out


def prep_kernel(dims, *refs):
    seq_count, head_count, small, rows, merged = dims
    counts_ref, before_ref, order_ref, kv_ref, rows_ref = refs[:5]
    block_ref, query_pos_ref, vit_bias_ref, vis_pos_ref, mine_ref, sem = refs[5:]
    seq, head = lax.axis_index("seq"), lax.axis_index("head")
    images = counts_ref.shape[0]
    half = mine_ref.shape[0]
    shift = pl.multiple_of(head * half, half) if head_count == 2 else 0
    copy = pltpu.make_async_copy(rows_ref.at[pl.ds(shift, half), :], mine_ref, sem)
    copy.start()

    tokens = order_ref.shape[1]
    order = order_ref[...]
    near = lax.broadcasted_iota(jnp.int32, (1, vit_bias_ref.shape[1]), 1)
    segments = [(0, 0), (rows, shift - rows), (rows + half, shift + rows)]
    if head_count == 2:
        other = half - shift
        segments += [(rows + 2 * half, other - rows), (rows + 3 * half, other + rows)]
    near = pick(near, segments) + seq * rows
    own = lax.broadcasted_iota(jnp.int32, (rows, 1), 0) + seq * rows
    vis = lax.broadcasted_iota(jnp.int32, vis_pos_ref.shape, 1)
    if small:
        segments = []
        for k in range(seq_count // 2):
            source = lax.rem(seq - 2 * k + seq_count, seq_count)
            partner = source + 1 - 2 * lax.rem(source, 2)
            segments += [(2 * k * merged, source * merged), ((2 * k + 1) * merged, partner * merged)]
        vis = pick(vis, segments)

    def step(i, state):
        pos, near_id, own_id, vis_pos, start, earlier = state
        count, before = counts_ref[i], before_ref[i]
        stop = start + count
        pos = pos + jnp.where(before <= order, count, 0)
        near_id = near_id + jnp.where(near >= 4 * stop, 1, 0)
        own_id = own_id + jnp.where(own >= 4 * stop, 1, 0)
        vis_pos = vis_pos + jnp.where(start <= vis, before - earlier, 0)
        return pos, near_id, own_id, vis_pos, stop, before

    zero = jnp.int32(0)
    state = (order, jnp.zeros_like(near), jnp.zeros_like(own), vis, zero, zero)
    if images <= 32:
        for i in range(images):
            state = step(i, state)
    else:
        state = lax.fori_loop(0, images, step, state)
    pos, near_id, own_id, vis_pos, _, _ = state
    near_id = jnp.where((near >= 0) & (near < rows * seq_count), near_id, -1)
    vit_bias_ref[...] = jnp.where(own_id == near_id, 0.0, masked_score)
    vis_pos_ref[...] = vis_pos.astype(f32)
    row = lax.broadcasted_iota(jnp.int32, (tokens, tokens), 0)
    column = lax.broadcasted_iota(jnp.int32, (tokens, tokens), 1)
    pos_row = pos.astype(f32)
    diagonal = jnp.where(row == column, pos_row, 0.0)
    query_pos_ref[...] = jnp.broadcast_to(jnp.sum(diagonal, axis=1, keepdims=True), query_pos_ref.shape)
    width = kv_ref.shape[2]
    block_ref[:tokens, :width] = kv_ref[:, 0, :]
    block_ref[:tokens, width:] = kv_ref[:, 1, :]
    high = jnp.floor(pos_row * (1.0 / 128.0))
    line = lax.broadcasted_iota(jnp.int32, (8, tokens), 0)
    tail = jnp.where(line == 0, high, jnp.where(line == 1, pos_row - 128.0 * high, 0.0))
    block_ref[tokens:, :tokens] = tail.astype(bf16)
    block_ref[tokens:, tokens:] = jnp.zeros((8, 2 * width - tokens), bf16)
    copy.wait()


def own_kernel(gain_ref, bias_ref, rows_ref, weight_ref, q_ref, k_ref, v_ref, wkv_ref, wq, sem):
    copies = [
        pltpu.make_async_copy(weight_ref.at[j], wq if j == 0 else wkv_ref.at[j - 1], sem.at[j]) for j in range(3)
    ]
    for copy in copies:
        copy.start()
    normed = layer_norm_rows([rows_ref], gain_ref, bias_ref)
    for j, out_ref in enumerate((q_ref, k_ref, v_ref)):
        copies[j].wait()
        weight = wq[...] if j == 0 else wkv_ref[j - 1]
        out_ref[...] = jnp.dot(normed, weight, preferred_element_type=f32).astype(bf16)


def near_kernel(gain_ref, bias_ref, weight_ref, *refs):
    normed = layer_norm_rows(refs[:-2], gain_ref, bias_ref)
    for j in range(2):
        refs[j - 2][...] = jnp.dot(normed, weight_ref[j], preferred_element_type=f32).astype(bf16)


def vit_kernel(parts, gain_ref, bias_ref, weight_ref, mask_ref, proj_ref, q_ref, *refs):
    key_refs, value_refs = refs[:parts], refs[parts : 2 * parts]
    row_refs = refs[2 * parts : -4]
    out_ref, keys, values, mixed = refs[-4:]
    row = 0
    for key_ref, value_ref in zip(key_refs, value_refs):
        n = key_ref.shape[0]
        keys[row : row + n, :] = key_ref[...]
        values[row : row + n, :] = value_ref[...]
        row += n
    if row_refs:
        normed = layer_norm_rows(row_refs, gain_ref, bias_ref)
        keys[row:, :] = jnp.dot(normed, weight_ref[0], preferred_element_type=f32).astype(bf16)
        values[row:, :] = jnp.dot(normed, weight_ref[1], preferred_element_type=f32).astype(bf16)
    head_cols = q_ref.shape[1]
    factor = math.log2(math.e) / math.sqrt(VIT_HD)
    for h in range(head_cols // VIT_HD):
        first, last = h * VIT_HD, (h + 1) * VIT_HD
        low, high = first // LANES * LANES, -(-last // LANES) * LANES
        column = low + lax.broadcasted_iota(jnp.int32, (1, high - low), 1)
        inside = (column >= first) & (column < last)
        query = jnp.where(inside, q_ref[:, low:high], jnp.zeros((), bf16))
        scores = lax.dot_general(
            query, keys[:, low:high], (((1,), (1,)), ((), ())), preferred_element_type=f32
        )
        scores = scores * factor + mask_ref[...]
        weights = jnp.exp2(scores - jnp.max(scores, axis=1, keepdims=True))
        total = jnp.sum(weights, axis=1, keepdims=True)
        part = jnp.dot(weights.astype(bf16), values[:, low:high], preferred_element_type=f32)
        part = (part * (1.0 / total)).astype(bf16)
        if first == low:
            mixed[:, low:high] = part
        else:
            split = low + LANES
            mixed[:, low:split] = jnp.where(inside[:, :LANES], part[:, :LANES], mixed[:, low:split])
            if high > split:
                mixed[:, split:high] = part[:, LANES:]
    out_ref[...] = jnp.dot(mixed[...], proj_ref[...], preferred_element_type=f32).astype(bf16)


def merge_kernel(rows_ref, mine_ref, other_ref, pbias_ref, gain_ref, bias_ref, weight_ref, out_ref, merged):
    rows, width = rows_ref.shape
    encoded = rows_ref[...].astype(f32) + (mine_ref[...].astype(f32) + other_ref[...].astype(f32))
    encoded = (encoded + pbias_ref[...].reshape(1, width)).astype(bf16).astype(f32)
    normed = layer_norm(encoded, gain_ref[...].reshape(1, width), bias_ref[...].reshape(1, width))
    for c in range(width // LANES):
        merged[c * rows : (c + 1) * rows, :] = normed[:, c * LANES : (c + 1) * LANES]
    total = None
    for i in range(4):
        piece = jnp.concatenate(
            [merged[pl.ds(c * rows + i, rows // 4, stride=4), :] for c in range(width // LANES)], axis=1
        ).astype(bf16)
        term = jnp.dot(piece, weight_ref[i * width : (i + 1) * width, :], preferred_element_type=f32)
        total = term if total is None else total + term
    out_ref[...] = total.astype(bf16)


def attention_kernel(tokens, blocks, chained, final, *refs):
    query_pos_ref, q_ref = refs[:2]
    refs = refs[2:]
    if tokens is None:
        pos_ref, refs = refs[0], refs[1:]
    block_refs, refs = refs[:blocks], refs[blocks:]
    state, refs = (refs[:3], refs[3:]) if chained else (None, refs)
    outs, (kv, va, bias) = refs[:-3], refs[-3:]
    row = 0
    for block_ref in block_refs:
        n = block_ref.shape[0]
        if tokens is None:
            kv[row : row + n, :] = block_ref[...]
            row += n
            continue
        for first in range(0, n, tokens + 8):
            kv[row : row + tokens, :] = block_ref[first : first + tokens, :]
            tail = block_ref[first + tokens : first + tokens + 8, :tokens].astype(f32)
            pos = tail[0:1, :] * 128.0 + tail[1:2, :]
            bias[:, row : row + tokens] = jnp.where(pos <= query_pos_ref[:, :tokens], 0.0, masked_score)
            row += tokens
    count = kv.shape[0]
    if tokens is None:
        bias[...] = jnp.where(pos_ref[...] <= query_pos_ref[:, :1], 0.0, masked_score)
    va[:, HEAD_DIM:] = jnp.ones((count, HEAD_DIM), bf16)
    heads = kv.shape[1] // (2 * HEAD_DIM)
    factor = math.log2(math.e) / math.sqrt(HEAD_DIM)
    for h in range(heads):
        keys = kv[:, h * HEAD_DIM : (h + 1) * HEAD_DIM]
        va[:, :HEAD_DIM] = kv[:, (heads + h) * HEAD_DIM : (heads + h + 1) * HEAD_DIM]
        for g in range(GROUP):
            columns = slice((h * GROUP + g) * HEAD_DIM, (h * GROUP + g + 1) * HEAD_DIM)
            scores = lax.dot_general(
                q_ref[:, columns], keys, (((1,), (1,)), ((), ())), preferred_element_type=f32
            )
            scores = scores * factor + bias[...]
            top = jnp.max(scores, axis=1, keepdims=True)
            if chained:
                wide = jnp.maximum(top, state[1][:, columns])
                copies = -(-count // HEAD_DIM)
                tops = jnp.concatenate([wide] * copies, axis=1)[:, :count] if copies > 1 else wide[:, :count]
                weights = jnp.exp2(scores - tops)
            else:
                wide = jnp.broadcast_to(top, (top.shape[0], HEAD_DIM))
                weights = jnp.exp2(scores - top)
            part = jnp.dot(weights.astype(bf16), va[...], preferred_element_type=f32)
            numer, denom = part[:, :HEAD_DIM], part[:, HEAD_DIM:]
            if chained:
                scale = jnp.exp2(state[1][:, columns] - wide)
                numer = numer + state[0][:, columns] * scale
                denom = denom + state[2][:, columns] * scale
            if final:
                outs[0][:, columns] = (numer / denom).astype(bf16)
            else:
                outs[0][:, columns] = numer
                outs[1][:, columns] = wide
                outs[2][:, columns] = denom


def attend(query_pos, queries, pos, blocks, state, tokens, final, name):
    rows, width = queries.shape
    if tokens is None:
        count = sum(block.shape[0] for block in blocks)
        head_args = (query_pos, queries, pos)
    else:
        count = sum(block.shape[0] // (tokens + 8) * tokens for block in blocks)
        head_args = (query_pos, queries)
    wide = jax.ShapeDtypeStruct((rows, width), f32)
    return vmem_call(
        functools.partial(attention_kernel, tokens, len(blocks), state is not None, final),
        jax.ShapeDtypeStruct((rows, width), bf16) if final else (wide, wide, wide),
        scratch=(
            pltpu.VMEM((count, blocks[0].shape[1]), bf16),
            pltpu.VMEM((count, 2 * HEAD_DIM), bf16),
            pltpu.VMEM((rows, count), f32),
        ),
        flops=4 * rows * width * count,
        nbytes=2 * queries.size + 2 * count * blocks[0].shape[1],
        trans=rows * width // HEAD_DIM * count,
        name=name,
    )(*head_args, *blocks, *(state or ()))


def per_device(
    patches,
    ln_gain,
    ln_bias,
    qkv_weight,
    proj_weight,
    proj_bias,
    merge_gain,
    merge_bias,
    visual_kv_weight,
    image_tokens,
    text_before,
    text_order,
    queries,
    text_kv,
):
    seq_count = lax.axis_size("seq")
    head_count = lax.axis_size("head")
    patch_rows, model_width = patches.shape
    merged_rows = patch_rows // 4
    head_cols = qkv_weight.shape[2]
    tokens = queries.shape[0]
    kv_width = text_kv.shape[1] * text_kv.shape[2]
    small = seq_count == 8 and head_count == 2
    half = patch_rows // 2 if head_count == 2 else patch_rows
    near_count = 3 * patch_rows

    block, query_pos, vit_bias, vis_pos, mine = vmem_call(
        functools.partial(prep_kernel, (seq_count, head_count, small, patch_rows, merged_rows)),
        (
            jax.ShapeDtypeStruct((tokens + 8, kv_width), bf16),
            jax.ShapeDtypeStruct((tokens, LANES), f32),
            jax.ShapeDtypeStruct((patch_rows, near_count), f32),
            jax.ShapeDtypeStruct((1, merged_rows * seq_count), f32),
            jax.ShapeDtypeStruct((half, model_width), bf16),
        ),
        scratch=(pltpu.SemaphoreType.DMA(()),),
        spaces={0: pltpu.SMEM, 1: pltpu.SMEM, 4: pl.ANY},
        flops=1 << 20,
        nbytes=1 << 20,
        name="prep",
    )(image_tokens, text_before, text_order[None, :], text_kv, patches)

    ahead = [(i, i + 1) for i in range(seq_count - 1)]
    back = [(i + 1, i) for i in range(seq_count - 1)]
    before_mine = lax.ppermute(mine, "seq", ahead)
    after_mine = lax.ppermute(mine, "seq", back)

    pair_swap = [(i, i ^ 1) for i in range(seq_count)]
    jumps = [[(i, (i + 2 * k) % seq_count) for i in range(seq_count)] for k in range(1, seq_count // 2)]
    if small:
        column = [block] + [lax.ppermute(block, "seq", jump) for jump in jumps]
        swapped = lax.ppermute(jnp.concatenate(column, axis=0), "seq", pair_swap)
        text_blocks = [column, [swapped]]
    else:
        gathered = lax.all_gather(block, "seq", axis=0, tiled=True)
        step = 8 * (tokens + 8)
        text_blocks = [[gathered[i : i + step]] for i in range(0, gathered.shape[0], step)]

    weight = jnp.transpose(qkv_weight, (1, 0, 2))
    cols = jax.ShapeDtypeStruct((patch_rows, head_cols), bf16)
    query, key_own, value_own, weight_kv = vmem_call(
        own_kernel,
        (cols, cols, cols, jax.ShapeDtypeStruct((2, model_width, head_cols), bf16)),
        scratch=(pltpu.VMEM((model_width, head_cols), bf16), pltpu.SemaphoreType.DMA((3,))),
        spaces={3: pl.ANY},
        flops=2 * patch_rows * weight.size,
        nbytes=2 * weight.size,
        name="own_qkv",
    )(ln_gain, ln_bias, patches, weight)

    near_cols = jax.ShapeDtypeStruct((2 * half, head_cols), bf16)
    key_near, value_near = vmem_call(
        near_kernel,
        (near_cols, near_cols),
        flops=4 * near_cols.shape[0] * model_width * head_cols,
        nbytes=2 * weight_kv.size,
        name="near_kv",
    )(ln_gain, ln_bias, weight_kv, before_mine, after_mine)
    others = ()
    if head_count == 2:
        head_swap = [(0, 1), (1, 0)]
        others = (lax.ppermute(before_mine, "head", head_swap), lax.ppermute(after_mine, "head", head_swap))
    mine_part = vmem_call(
        functools.partial(vit_kernel, 2),
        jax.ShapeDtypeStruct((patch_rows, model_width), bf16),
        scratch=(
            pltpu.VMEM((near_count, head_cols), bf16),
            pltpu.VMEM((near_count, head_cols), bf16),
            pltpu.VMEM((patch_rows, head_cols), bf16),
        ),
        flops=4 * patch_rows * near_count * head_cols + 2 * patch_rows * head_cols * model_width,
        nbytes=2 * proj_weight.size,
        trans=patch_rows * near_count * head_cols // VIT_HD,
        name="vit_attention",
    )(
        ln_gain, ln_bias, weight_kv, vit_bias, proj_weight, query, key_own, key_near, value_own, value_near, *others
    )
    if head_count == 2:
        other_part = lax.ppermute(mine_part, "head", head_swap)
    else:
        other_part = lax.psum(mine_part, "head") - mine_part
    map_weight = visual_kv_weight.reshape(4 * model_width, -1)
    visual = vmem_call(
        merge_kernel,
        jax.ShapeDtypeStruct((merged_rows, kv_width), bf16),
        scratch=(pltpu.VMEM((patch_rows * (model_width // LANES), LANES), f32),),
        flops=2 * merged_rows * map_weight.size,
        nbytes=2 * map_weight.size,
        name="merge",
    )(patches, mine_part, other_part, proj_bias, merge_gain, merge_bias, map_weight)

    if small:
        pair = jnp.concatenate([visual, lax.ppermute(visual, "seq", pair_swap)])
        visual_blocks = [[pair] + [lax.ppermute(pair, "seq", jump) for jump in jumps]]
    else:
        gathered = lax.all_gather(visual, "seq", axis=0, tiled=True)
        step = 8 * merged_rows
        visual_blocks = [[gathered[i : i + step]] for i in range(0, gathered.shape[0], step)]

    state = None
    for text_block in text_blocks:
        state = attend(query_pos, queries, None, text_block, state, tokens, False, "text_part")
    first = 0
    for i, visual_block in enumerate(visual_blocks):
        count = sum(b.shape[0] for b in visual_block)
        final = i == len(visual_blocks) - 1
        pos = vis_pos[:, first : first + count]
        state = attend(query_pos, queries, pos, visual_block, state, None, final, "visual_part")
        first += count
    return (state, visual.reshape(merged_rows, text_kv.shape[1], -1))


def solution(mesh):
    in_specs = (
        P(("grp", "seq"), None),
        P(),
        P(),
        P(None, None, "head"),
        P("head", None),
        P(),
        P(),
        P(),
        P(None, None, "head"),
        P("grp"),
        P("grp"),
        P(("grp", "seq")),
        P(("grp", "seq"), "head"),
        P(("grp", "seq"), None, "head"),
    )
    out_specs = (P(("grp", "seq"), "head"), P(("grp", "seq"), None, "head"))
    return jax.shard_map(
        per_device, mesh=mesh, in_specs=in_specs, out_specs=out_specs, check_vma=False
    )
```

```python
import functools
import math

import jax
import jax.numpy as jnp
from jax import lax
from jax.experimental import pallas as pl
from jax.experimental.pallas import tpu as pltpu
from jax.sharding import PartitionSpec as P


VIT_HD = 80
HEAD_DIM = 128
GROUP = 8
LANES = 128

epsilon = 1e-06
SHIFTS = (2, 4, 6, 1, 7, 3, 5)
masked_score = -1e30


f32 = jnp.float32
bf16 = jnp.bfloat16


def layer_norm(inputs, scale_gain, shift_bias):
    centre = jnp.mean(inputs, axis=-1, keepdims=True)
    centred = inputs - centre
    spread = jnp.mean(centred * centred, axis=-1, keepdims=True)
    return centred * lax.rsqrt(spread + epsilon) * scale_gain + shift_bias


def padded_bytes(shape, dtype):
    item = jnp.dtype(dtype).itemsize
    rows = shape[-2] if len(shape) > 1 else 1
    count = math.prod(shape[:-2]) * (-(-rows // 16) * 16) * (-(-shape[-1] // LANES) * LANES)
    return count * item


def vmem_call(body, out_shape, scratch=(), flops=0, nbytes=0, trans=0, spaces=None, spare=6 << 20, keep=False):
    spaces = spaces or {}

    def run(*args):
        args = [pltpu.with_memory_space_constraint(a, pltpu.HBM) if spaces.get(i) == pltpu.HBM else a for i, a in enumerate(args)]
        multi = isinstance(out_shape, (tuple, list))
        size = sum(padded_bytes(a.shape, a.dtype) for a in scratch if a.memory_space == pltpu.VMEM)
        spec = pl.BlockSpec(memory_space=pltpu.VMEM)
        return pl.pallas_call(
            body,
            out_shape=jax.tree.map(lambda a: pltpu.VMEM(a.shape, a.dtype), out_shape) if keep else out_shape,
            in_specs=[pl.BlockSpec(memory_space=spaces.get(i, pltpu.VMEM)) for i in range(len(args))],
            out_specs=[spec] * len(out_shape) if multi else spec,
            scratch_shapes=scratch,
            compiler_params=pltpu.CompilerParams(vmem_limit_bytes=size + spare),
            cost_estimate=pl.CostEstimate(flops=flops, bytes_accessed=nbytes, transcendentals=trans),
        )(*args)

    return run


def layer_norm_rows(refs, gain_ref, bias_ref):
    width = gain_ref.shape[0]
    rows = jnp.concatenate([ref[...] for ref in refs], axis=0).astype(f32)
    return layer_norm(rows, gain_ref[...].reshape(1, width), bias_ref[...].reshape(1, width)).astype(bf16)


def pick(index, segments):
    out = index + segments[0][1]
    for offset, start in segments[1:]:
        out = jnp.where(index >= offset, index - offset + start, out)
    return out


def prep_kernel(dims, *refs):
    seq_count, small, rows, merged = dims
    sources, outs, held, sem = refs[:4], refs[4:8], refs[8:12], refs[12]
    copies = [pltpu.make_async_copy(a, b, sem.at[i]) for i, (a, b) in enumerate(zip(sources, held))]
    for copy in copies:
        copy.start()
    for copy in copies:
        copy.wait()
    counts_ref, before_ref, order_ref, kv_ref = held
    block_ref, query_pos_ref, vit_bias_ref, vis_pos_ref = outs
    seq, head = lax.axis_index("seq"), lax.axis_index("head")
    images = counts_ref.shape[0]
    tokens = order_ref.shape[1]
    order = order_ref[...]
    near = lax.broadcasted_iota(jnp.int32, (1, vit_bias_ref.shape[1]), 1)
    first = rows * (2 * head - 1)
    segments = [(0, 0), (rows, first), (2 * rows, -first)]
    near = pick(near, segments) + seq * rows
    own = lax.broadcasted_iota(jnp.int32, (rows, 1), 0) + seq * rows
    vis = lax.broadcasted_iota(jnp.int32, vis_pos_ref.shape, 1)
    if small:
        segments = [(0, seq * merged)]
        for i, k in enumerate(SHIFTS):
            segments.append(((i + 1) * merged, lax.rem(seq - k + seq_count, seq_count) * merged))
        vis = pick(vis, segments)

    def step(i, state):
        pos, near_id, own_id, vis_pos, start, earlier = state
        count, before = counts_ref[i], before_ref[i]
        stop = start + count
        pos = pos + jnp.where(before <= order, count, 0)
        near_id = near_id + jnp.where(near >= 4 * stop, 1, 0)
        own_id = own_id + jnp.where(own >= 4 * stop, 1, 0)
        vis_pos = vis_pos + jnp.where(start <= vis, before - earlier, 0)
        return pos, near_id, own_id, vis_pos, stop, before

    zero = jnp.int32(0)
    state = (order, jnp.zeros_like(near), jnp.zeros_like(own), vis, zero, zero)
    if images <= 32:
        for i in range(images):
            state = step(i, state)
    else:
        state = lax.fori_loop(0, images, step, state)
    pos, near_id, own_id, vis_pos, _, _ = state
    near_id = jnp.where((near >= 0) & (near < rows * seq_count), near_id, -1)
    vit_bias_ref[...] = jnp.where(own_id == near_id, 0.0, masked_score)
    vis_pos_ref[...] = vis_pos.astype(f32)
    row = lax.broadcasted_iota(jnp.int32, (tokens, tokens), 0)
    column = lax.broadcasted_iota(jnp.int32, (tokens, tokens), 1)
    pos_row = pos.astype(f32)
    diagonal = jnp.where(row == column, pos_row, 0.0)
    query_pos_ref[...] = jnp.broadcast_to(jnp.sum(diagonal, axis=1, keepdims=True), query_pos_ref.shape)
    width = kv_ref.shape[2]
    block_ref[:tokens, :width] = kv_ref[:, 0, :]
    block_ref[:tokens, width:] = kv_ref[:, 1, :]
    high = jnp.floor(pos_row * (1.0 / 128.0))
    line = lax.broadcasted_iota(jnp.int32, (8, tokens), 0)
    tail = jnp.where(line == 0, high, jnp.where(line == 1, pos_row - 128.0 * high, 0.0))
    block_ref[tokens:, :tokens] = tail.astype(bf16)
    block_ref[tokens:, tokens:] = jnp.zeros((8, 2 * width - tokens), bf16)


def own_kernel(carried, weight_ref, *refs):
    sources, refs = refs[:carried], refs[carried:]
    q_ref, k_ref, v_ref, wkv_ref = refs[:4]
    kept, (wq, sem) = refs[4:-2], refs[-2:]
    pairs = list(zip(sources[:3], kept[:3]))
    pairs += [(weight_ref.at[j], wq if j == 0 else wkv_ref.at[j - 1]) for j in range(3)]
    pairs += list(zip(sources[3:], kept[3:]))
    copies = [pltpu.make_async_copy(a, b, sem.at[i]) for i, (a, b) in enumerate(pairs)]
    for copy in copies:
        copy.start()
    for copy in copies[:3]:
        copy.wait()
    normed = layer_norm_rows(kept[:1], kept[1], kept[2])
    for j, out_ref in enumerate((q_ref, k_ref, v_ref)):
        copies[3 + j].wait()
        weight = wq[...] if j == 0 else wkv_ref[j - 1]
        out_ref[...] = jnp.dot(normed, weight, preferred_element_type=f32).astype(bf16)
    for copy in copies[6:]:
        copy.wait()


def near_kernel(gain_ref, bias_ref, weight_ref, *refs):
    normed = layer_norm_rows(refs[:-2], gain_ref, bias_ref)
    for j in range(2):
        refs[j - 2][...] = jnp.dot(normed, weight_ref[j], preferred_element_type=f32).astype(bf16)


def vit_kernel(parts, gain_ref, bias_ref, weight_ref, mask_ref, proj_ref, q_ref, *refs):
    key_refs, value_refs = refs[:parts], refs[parts : 2 * parts]
    row_refs = refs[2 * parts : -4]
    out_ref, keys, values, mixed = refs[-4:]
    row = 0
    for key_ref, value_ref in zip(key_refs, value_refs):
        n = key_ref.shape[0]
        keys[row : row + n, :] = key_ref[...]
        values[row : row + n, :] = value_ref[...]
        row += n
    if row_refs:
        normed = layer_norm_rows(row_refs, gain_ref, bias_ref)
        keys[row:, :] = jnp.dot(normed, weight_ref[0], preferred_element_type=f32).astype(bf16)
        values[row:, :] = jnp.dot(normed, weight_ref[1], preferred_element_type=f32).astype(bf16)
    head_cols = q_ref.shape[1]
    factor = math.log2(math.e) / math.sqrt(VIT_HD)
    for h in range(head_cols // VIT_HD):
        first, last = h * VIT_HD, (h + 1) * VIT_HD
        low, high = first // LANES * LANES, -(-last // LANES) * LANES
        column = low + lax.broadcasted_iota(jnp.int32, (1, high - low), 1)
        inside = (column >= first) & (column < last)
        query = jnp.where(inside, q_ref[:, low:high], jnp.zeros((), bf16))
        scores = lax.dot_general(
            query, keys[:, low:high], (((1,), (1,)), ((), ())), preferred_element_type=f32
        )
        scores = scores * factor + mask_ref[...]
        weights = jnp.exp2(scores - jnp.max(scores, axis=1, keepdims=True))
        total = jnp.sum(weights, axis=1, keepdims=True)
        part = jnp.dot(weights.astype(bf16), values[:, low:high], preferred_element_type=f32)
        part = (part * (1.0 / total)).astype(bf16)
        if first == low:
            mixed[:, low:high] = part
        else:
            split = low + LANES
            mixed[:, low:split] = jnp.where(inside[:, :LANES], part[:, :LANES], mixed[:, low:split])
            if high > split:
                mixed[:, split:high] = part[:, LANES:]
    out_ref[...] = jnp.dot(mixed[...], proj_ref[...], preferred_element_type=f32).astype(bf16)


def merge_kernel(rows_ref, mine_ref, other_ref, pbias_ref, gain_ref, bias_ref, weight_ref, out_ref, merged):
    rows, width = rows_ref.shape
    encoded = rows_ref[...].astype(f32) + (mine_ref[...].astype(f32) + other_ref[...].astype(f32))
    encoded = (encoded + pbias_ref[...].reshape(1, width)).astype(bf16).astype(f32)
    normed = layer_norm(encoded, gain_ref[...].reshape(1, width), bias_ref[...].reshape(1, width))
    for c in range(width // LANES):
        merged[c * rows : (c + 1) * rows, :] = normed[:, c * LANES : (c + 1) * LANES]
    total = None
    for i in range(4):
        piece = jnp.concatenate(
            [merged[pl.ds(c * rows + i, rows // 4, stride=4), :] for c in range(width // LANES)], axis=1
        ).astype(bf16)
        term = jnp.dot(piece, weight_ref[i * width : (i + 1) * width, :], preferred_element_type=f32)
        total = term if total is None else total + term
    out_ref[...] = total.astype(bf16)


def attention_kernel(tokens, blocks, chained, final, *refs):
    query_pos_ref, q_ref = refs[:2]
    refs = refs[2:]
    if tokens is None:
        pos_ref, refs = refs[0], refs[1:]
    block_refs, refs = refs[:blocks], refs[blocks:]
    state, refs = (refs[:3], refs[3:]) if chained else (None, refs)
    outs, (kv, va, bias) = refs[:-3], refs[-3:]
    row = 0
    for block_ref in block_refs:
        n = block_ref.shape[0]
        if tokens is None:
            kv[row : row + n, :] = block_ref[...]
            row += n
            continue
        for first in range(0, n, tokens + 8):
            kv[row : row + tokens, :] = block_ref[first : first + tokens, :]
            tail = block_ref[first + tokens : first + tokens + 8, :tokens].astype(f32)
            pos = tail[0:1, :] * 128.0 + tail[1:2, :]
            bias[:, row : row + tokens] = jnp.where(pos <= query_pos_ref[:, :tokens], 0.0, masked_score)
            row += tokens
    count = kv.shape[0]
    if tokens is None:
        bias[...] = jnp.where(pos_ref[...] <= query_pos_ref[:, :1], 0.0, masked_score)
    va[:, HEAD_DIM:] = jnp.ones((count, HEAD_DIM), bf16)
    heads = kv.shape[1] // (2 * HEAD_DIM)
    factor = math.log2(math.e) / math.sqrt(HEAD_DIM)
    for h in range(heads):
        keys = kv[:, h * HEAD_DIM : (h + 1) * HEAD_DIM]
        va[:, :HEAD_DIM] = kv[:, (heads + h) * HEAD_DIM : (heads + h + 1) * HEAD_DIM]
        for g in range(GROUP):
            columns = slice((h * GROUP + g) * HEAD_DIM, (h * GROUP + g + 1) * HEAD_DIM)
            scores = lax.dot_general(
                q_ref[:, columns], keys, (((1,), (1,)), ((), ())), preferred_element_type=f32
            )
            scores = scores * factor + bias[...]
            top = jnp.max(scores, axis=1, keepdims=True)
            if chained:
                wide = jnp.maximum(top, state[1][:, columns])
                copies = -(-count // HEAD_DIM)
                tops = jnp.concatenate([wide] * copies, axis=1)[:, :count] if copies > 1 else wide[:, :count]
                weights = jnp.exp2(scores - tops)
            else:
                wide = jnp.broadcast_to(top, (top.shape[0], HEAD_DIM))
                weights = jnp.exp2(scores - top)
            part = jnp.dot(weights.astype(bf16), va[...], preferred_element_type=f32)
            numer, denom = part[:, :HEAD_DIM], part[:, HEAD_DIM:]
            if chained:
                scale = jnp.exp2(state[1][:, columns] - wide)
                numer = numer + state[0][:, columns] * scale
                denom = denom + state[2][:, columns] * scale
            if final:
                outs[0][:, columns] = (numer / denom).astype(bf16)
            else:
                outs[0][:, columns] = numer
                outs[1][:, columns] = wide
                outs[2][:, columns] = denom


def join_kernel(*refs):
    row = 0
    for ref in refs[:-1]:
        refs[-1][row : row + ref.shape[0], :] = ref[...]
        row += ref.shape[0]


def join(blocks):
    rows = sum(block.shape[0] for block in blocks)
    return vmem_call(
        join_kernel,
        jax.ShapeDtypeStruct((rows, blocks[0].shape[1]), blocks[0].dtype),
        flops=1 << 16,
        nbytes=4 * rows * blocks[0].shape[1],
    )(*blocks)


def attend(query_pos, queries, pos, blocks, state, tokens, final):
    rows, width = queries.shape
    if tokens is None:
        count = sum(block.shape[0] for block in blocks)
        head_args = (query_pos, queries, pos)
    else:
        count = sum(block.shape[0] // (tokens + 8) * tokens for block in blocks)
        head_args = (query_pos, queries)
    wide = jax.ShapeDtypeStruct((rows, width), f32)
    return vmem_call(
        functools.partial(attention_kernel, tokens, len(blocks), state is not None, final),
        jax.ShapeDtypeStruct((rows, width), bf16) if final else (wide, wide, wide),
        scratch=(
            pltpu.VMEM((count, blocks[0].shape[1]), bf16),
            pltpu.VMEM((count, 2 * HEAD_DIM), bf16),
            pltpu.VMEM((rows, count), f32),
        ),
        flops=4 * rows * width * count,
        nbytes=2 * queries.size + 2 * count * blocks[0].shape[1],
        trans=rows * width // HEAD_DIM * count,
        keep=not final,
    )(*head_args, *blocks, *(state or ()))


def per_device(
    patches,
    ln_gain,
    ln_bias,
    qkv_weight,
    proj_weight,
    proj_bias,
    merge_gain,
    merge_bias,
    visual_kv_weight,
    image_tokens,
    text_before,
    text_order,
    queries,
    text_kv,
):
    seq_count = lax.axis_size("seq")
    head_count = lax.axis_size("head")
    patch_rows, model_width = patches.shape
    merged_rows = patch_rows // 4
    head_cols = qkv_weight.shape[2]
    tokens = queries.shape[0]
    kv_width = text_kv.shape[1] * text_kv.shape[2]
    small = is_small(seq_count, head_count)
    near_count = 3 * patch_rows
    share = jax.ShapeDtypeStruct

    ahead = [(2 * i, 2 * i + 2) for i in range(seq_count - 1)]
    back = [(2 * i + 3, 2 * i + 1) for i in range(seq_count - 1)]
    near_first = lax.ppermute(patches, ("seq", "head"), ahead + back)

    block, query_pos, vit_bias, vis_pos = vmem_call(
        functools.partial(prep_kernel, (seq_count, small, patch_rows, merged_rows)),
        (
            share((tokens + 8, kv_width), bf16),
            share((tokens, LANES), f32),
            share((patch_rows, near_count), f32),
            share((1, merged_rows * seq_count), f32),
        ),
        scratch=(
            pltpu.SMEM(image_tokens.shape, jnp.int32),
            pltpu.SMEM(text_before.shape, jnp.int32),
            pltpu.VMEM((1, tokens), jnp.int32),
            pltpu.VMEM(text_kv.shape, bf16),
            pltpu.SemaphoreType.DMA((4,)),
        ),
        spaces={i: pltpu.HBM for i in range(4)},
        flops=1 << 20,
        nbytes=1 << 20,
    )(image_tokens, text_before, text_order[None, :], text_kv)
    pair_swap = [(i, i ^ 1) for i in range(seq_count)]
    jumps = [[(i, (i + 2 * k) % seq_count) for i in range(seq_count)] for k in range(1, seq_count // 2)]
    if small:
        column = [block]
        for jump in jumps:
            column.append(lax.ppermute(block, "seq", jump))
        column.append(lax.ppermute(block, "seq", pair_swap))
        pieces = join(column[1:4])
        column.append(lax.ppermute(pieces, "seq", pair_swap))
        text_blocks = [column]
    else:
        gathered = lax.all_gather(block, "seq", axis=0, tiled=True)
        step = 8 * (tokens + 8)
        text_blocks = [[gathered[i : i + step]] for i in range(0, gathered.shape[0], step)]

    weight = jnp.transpose(qkv_weight, (1, 0, 2))
    cols = share((patch_rows, head_cols), bf16)
    carried = [patches, ln_gain, ln_bias, proj_bias, merge_gain, merge_bias]
    query, key_own, value_own, weight_kv, *carried = vmem_call(
        functools.partial(own_kernel, len(carried)),
        (cols, cols, cols, share((2, model_width, head_cols), bf16), *[share(a.shape, a.dtype) for a in carried]),
        scratch=(pltpu.VMEM((model_width, head_cols), bf16), pltpu.SemaphoreType.DMA((3 + len(carried),))),
        spaces={i: pltpu.HBM for i in range(1 + len(carried))},
        flops=2 * patch_rows * weight.size,
        nbytes=2 * weight.size,
    )(weight, *carried)
    patches, ln_gain, ln_bias, proj_bias, merge_gain, merge_bias = carried

    key_near, value_near = vmem_call(
        near_kernel, (cols, cols), flops=4 * patch_rows * model_width * head_cols, nbytes=2 * weight_kv.size
    )(ln_gain, ln_bias, weight_kv, near_first)
    head_swap = [(0, 1), (1, 0)]
    near_second = lax.ppermute(near_first, "head", head_swap)
    mine_part = vmem_call(
        functools.partial(vit_kernel, 2),
        share((patch_rows, model_width), bf16),
        scratch=(
            pltpu.VMEM((near_count, head_cols), bf16),
            pltpu.VMEM((near_count, head_cols), bf16),
            pltpu.VMEM((patch_rows, head_cols), bf16),
        ),
        flops=4 * patch_rows * near_count * head_cols + 2 * patch_rows * head_cols * model_width,
        nbytes=2 * proj_weight.size,
        trans=patch_rows * near_count * head_cols // VIT_HD,
    )(ln_gain, ln_bias, weight_kv, vit_bias, proj_weight, query, key_own, key_near, value_own, value_near, near_second)
    other_part = lax.ppermute(mine_part, "head", head_swap)
    map_weight = visual_kv_weight.reshape(4 * model_width, -1)
    visual = vmem_call(
        merge_kernel,
        share((merged_rows, kv_width), bf16),
        scratch=(pltpu.VMEM((patch_rows * (model_width // LANES), LANES), f32),),
        flops=2 * merged_rows * map_weight.size,
        nbytes=2 * map_weight.size,
    )(patches, mine_part, other_part, proj_bias, merge_gain, merge_bias, map_weight)

    if small:
        visual_blocks = [[visual]]
        for k in SHIFTS:
            visual_blocks[0].append(lax.ppermute(visual, "seq", [(i, (i + k) % 8) for i in range(8)]))
    else:
        gathered = lax.all_gather(visual, "seq", axis=0, tiled=True)
        step = 8 * merged_rows
        visual_blocks = [[gathered[i : i + step]] for i in range(0, gathered.shape[0], step)]

    state = None
    for text_block in text_blocks:
        state = attend(query_pos, queries, None, text_block, state, tokens, False)
    first = 0
    for i, visual_block in enumerate(visual_blocks):
        count = sum(b.shape[0] for b in visual_block)
        final = i == len(visual_blocks) - 1
        pos = vis_pos[:, first : first + count]
        state = attend(query_pos, queries, pos, visual_block, state, None, final)
        first += count
    return (state, visual.reshape(merged_rows, text_kv.shape[1], -1))


def is_small(seq_count, head_count):
    return seq_count == 8 and head_count == 2


def solution(mesh):
    in_specs = (
        P(("grp", "seq"), None),
        P(),
        P(),
        P(None, None, "head"),
        P("head", None),
        P(),
        P(),
        P(),
        P(None, None, "head"),
        P("grp"),
        P("grp"),
        P(("grp", "seq")),
        P(("grp", "seq"), "head"),
        P(("grp", "seq"), None, "head"),
    )
    out_specs = (P(("grp", "seq"), "head"), P(("grp", "seq"), None, "head"))

    return jax.shard_map(per_device, mesh=mesh, in_specs=in_specs, out_specs=out_specs, check_vma=False)
```

```python
import functools
import math

import jax
import jax.numpy as jnp
from jax import lax
from jax.experimental import pallas as pl
from jax.experimental.pallas import tpu as pltpu
from jax.sharding import PartitionSpec as P


VIT_HD = 80
HEAD_DIM = 128
GROUP = 8
LANES = 128

epsilon = 1e-06

SHIFTS = (6, 4, 7, 5, 3, 2, 1)
masked_score = -1e30


f32 = jnp.float32
bf16 = jnp.bfloat16


def layer_norm(inputs, scale_gain, shift_bias):
    centre = jnp.mean(inputs, axis=-1, keepdims=True)
    centred = inputs - centre
    spread = jnp.mean(centred * centred, axis=-1, keepdims=True)
    return centred * lax.rsqrt(spread + epsilon) * scale_gain + shift_bias


def padded_bytes(shape, dtype):
    item = jnp.dtype(dtype).itemsize
    rows = shape[-2] if len(shape) > 1 else 1
    count = math.prod(shape[:-2]) * (-(-rows // 16) * 16) * (-(-shape[-1] // LANES) * LANES)
    return count * item


def vmem_call(body, out_shape, scratch=(), flops=0, nbytes=0, trans=0, spaces=None, spare=6 << 20, keep=False):
    spaces = spaces or {}

    def run(*args):
        args = [pltpu.with_memory_space_constraint(a, pltpu.HBM) if spaces.get(i) == pltpu.HBM else a for i, a in enumerate(args)]
        multi = isinstance(out_shape, (tuple, list))
        size = sum(padded_bytes(a.shape, a.dtype) for a in scratch if a.memory_space == pltpu.VMEM)
        spec = pl.BlockSpec(memory_space=pltpu.VMEM)
        return pl.pallas_call(
            body,
            out_shape=jax.tree.map(lambda a: pltpu.VMEM(a.shape, a.dtype), out_shape) if keep else out_shape,
            in_specs=[pl.BlockSpec(memory_space=spaces.get(i, pltpu.VMEM)) for i in range(len(args))],
            out_specs=[spec] * len(out_shape) if multi else spec,
            scratch_shapes=scratch,
            compiler_params=pltpu.CompilerParams(vmem_limit_bytes=size + spare),
            cost_estimate=pl.CostEstimate(flops=flops, bytes_accessed=nbytes, transcendentals=trans),
        )(*args)

    return run


def layer_norm_rows(refs, gain_ref, bias_ref):
    width = gain_ref.shape[0]
    rows = jnp.concatenate([ref[...] for ref in refs], axis=0).astype(f32)
    return layer_norm(rows, gain_ref[...].reshape(1, width), bias_ref[...].reshape(1, width)).astype(bf16)


def pick(index, segments):
    out = index + segments[0][1]
    for offset, start in segments[1:]:
        out = jnp.where(index >= offset, index - offset + start, out)
    return out


def prep_kernel(dims, *refs):
    seq_count, small, rows, merged = dims
    sources, outs, held, sem = refs[:4], refs[4:8], refs[8:12], refs[12]
    copies = [pltpu.make_async_copy(a, b, sem.at[i]) for i, (a, b) in enumerate(zip(sources, held))]
    for copy in copies:
        copy.start()
    for copy in copies:
        copy.wait()
    counts_ref, before_ref, order_ref, kv_ref = held
    block_ref, query_pos_ref, vit_bias_ref, vis_pos_ref = outs
    seq, head = lax.axis_index("seq"), lax.axis_index("head")
    images = counts_ref.shape[0]
    tokens = order_ref.shape[1]
    order = order_ref[...]
    near = lax.broadcasted_iota(jnp.int32, (1, vit_bias_ref.shape[1]), 1)
    first = rows * (2 * head - 1)
    segments = [(0, 0), (rows, first), (2 * rows, -first)]
    near = pick(near, segments) + seq * rows
    own = lax.broadcasted_iota(jnp.int32, (rows, 1), 0) + seq * rows
    vis = lax.broadcasted_iota(jnp.int32, vis_pos_ref.shape, 1)
    if small:
        segments = [(0, seq * merged)]
        for i, k in enumerate(SHIFTS):
            segments.append(((i + 1) * merged, lax.bitwise_xor(seq, jnp.int32(k)) * merged))
        vis = pick(vis, segments)

    def step(i, state):
        pos, near_id, own_id, vis_pos, start, earlier = state
        count, before = counts_ref[i], before_ref[i]
        stop = start + count
        pos = pos + jnp.where(before <= order, count, 0)
        near_id = near_id + jnp.where(near >= 4 * stop, 1, 0)
        own_id = own_id + jnp.where(own >= 4 * stop, 1, 0)
        vis_pos = vis_pos + jnp.where(start <= vis, before - earlier, 0)
        return pos, near_id, own_id, vis_pos, stop, before

    zero = jnp.int32(0)
    state = (order, jnp.zeros_like(near), jnp.zeros_like(own), vis, zero, zero)
    if images <= 32:
        for i in range(images):
            state = step(i, state)
    else:
        state = lax.fori_loop(0, images, step, state)
    pos, near_id, own_id, vis_pos, _, _ = state
    near_id = jnp.where((near >= 0) & (near < rows * seq_count), near_id, -1)
    vit_bias_ref[...] = jnp.where(own_id == near_id, 0.0, masked_score)
    vis_pos_ref[...] = vis_pos.astype(f32)
    row = lax.broadcasted_iota(jnp.int32, (tokens, tokens), 0)
    column = lax.broadcasted_iota(jnp.int32, (tokens, tokens), 1)
    pos_row = pos.astype(f32)
    diagonal = jnp.where(row == column, pos_row, 0.0)
    query_pos_ref[...] = jnp.broadcast_to(jnp.sum(diagonal, axis=1, keepdims=True), query_pos_ref.shape)
    width = kv_ref.shape[2]
    block_ref[:tokens, :width] = kv_ref[:, 0, :]
    block_ref[:tokens, width:] = kv_ref[:, 1, :]
    high = jnp.floor(pos_row * (1.0 / 128.0))
    line = lax.broadcasted_iota(jnp.int32, (8, tokens), 0)
    tail = jnp.where(line == 0, high, jnp.where(line == 1, pos_row - 128.0 * high, 0.0))
    block_ref[tokens:, :tokens] = tail.astype(bf16)
    block_ref[tokens:, tokens:] = jnp.zeros((8, 2 * width - tokens), bf16)


def own_kernel(carried, weight_ref, *refs):
    sources, refs = refs[:carried], refs[carried:]
    q_ref, k_ref, v_ref, wkv_ref = refs[:4]
    kept, (wq, sem) = refs[4:-2], refs[-2:]
    pairs = list(zip(sources[:3], kept[:3]))
    pairs += [(weight_ref.at[j], wq if j == 0 else wkv_ref.at[j - 1]) for j in range(3)]
    pairs += list(zip(sources[3:], kept[3:]))
    copies = [pltpu.make_async_copy(a, b, sem.at[i]) for i, (a, b) in enumerate(pairs)]
    for copy in copies:
        copy.start()
    for copy in copies[:3]:
        copy.wait()
    normed = layer_norm_rows(kept[:1], kept[1], kept[2])
    for j, out_ref in enumerate((q_ref, k_ref, v_ref)):
        copies[3 + j].wait()
        weight = wq[...] if j == 0 else wkv_ref[j - 1]
        out_ref[...] = jnp.dot(normed, weight, preferred_element_type=f32).astype(bf16)
    for copy in copies[6:]:
        copy.wait()


def near_kernel(gain_ref, bias_ref, weight_ref, *refs):
    normed = layer_norm_rows(refs[:-2], gain_ref, bias_ref)
    for j in range(2):
        refs[j - 2][...] = jnp.dot(normed, weight_ref[j], preferred_element_type=f32).astype(bf16)


def vit_kernel(parts, gain_ref, bias_ref, weight_ref, mask_ref, proj_ref, q_ref, *refs):
    key_refs, value_refs = refs[:parts], refs[parts : 2 * parts]
    row_refs = refs[2 * parts : -4]
    out_ref, keys, values, mixed = refs[-4:]
    row = 0
    for key_ref, value_ref in zip(key_refs, value_refs):
        n = key_ref.shape[0]
        keys[row : row + n, :] = key_ref[...]
        values[row : row + n, :] = value_ref[...]
        row += n
    if row_refs:
        normed = layer_norm_rows(row_refs, gain_ref, bias_ref)
        keys[row:, :] = jnp.dot(normed, weight_ref[0], preferred_element_type=f32).astype(bf16)
        values[row:, :] = jnp.dot(normed, weight_ref[1], preferred_element_type=f32).astype(bf16)
    head_cols = q_ref.shape[1]
    factor = math.log2(math.e) / math.sqrt(VIT_HD)
    for h in range(head_cols // VIT_HD):
        first, last = h * VIT_HD, (h + 1) * VIT_HD
        low, high = first // LANES * LANES, -(-last // LANES) * LANES
        column = low + lax.broadcasted_iota(jnp.int32, (1, high - low), 1)
        inside = (column >= first) & (column < last)
        query = jnp.where(inside, q_ref[:, low:high], jnp.zeros((), bf16))
        scores = lax.dot_general(
            query, keys[:, low:high], (((1,), (1,)), ((), ())), preferred_element_type=f32
        )
        scores = scores * factor + mask_ref[...]
        weights = jnp.exp2(scores - jnp.max(scores, axis=1, keepdims=True))
        total = jnp.sum(weights, axis=1, keepdims=True)
        part = jnp.dot(weights.astype(bf16), values[:, low:high], preferred_element_type=f32)
        part = (part * (1.0 / total)).astype(bf16)
        if first == low:
            mixed[:, low:high] = part
        else:
            split = low + LANES
            mixed[:, low:split] = jnp.where(inside[:, :LANES], part[:, :LANES], mixed[:, low:split])
            if high > split:
                mixed[:, split:high] = part[:, LANES:]
    out_ref[...] = jnp.dot(mixed[...], proj_ref[...], preferred_element_type=f32).astype(bf16)


def merge_kernel(rows_ref, mine_ref, other_ref, pbias_ref, gain_ref, bias_ref, weight_ref, out_ref, merged):
    rows, width = rows_ref.shape
    encoded = rows_ref[...].astype(f32) + (mine_ref[...].astype(f32) + other_ref[...].astype(f32))
    encoded = (encoded + pbias_ref[...].reshape(1, width)).astype(bf16).astype(f32)
    normed = layer_norm(encoded, gain_ref[...].reshape(1, width), bias_ref[...].reshape(1, width))
    for c in range(width // LANES):
        merged[c * rows : (c + 1) * rows, :] = normed[:, c * LANES : (c + 1) * LANES]
    total = None
    for i in range(4):
        piece = jnp.concatenate(
            [merged[pl.ds(c * rows + i, rows // 4, stride=4), :] for c in range(width // LANES)], axis=1
        ).astype(bf16)
        term = jnp.dot(piece, weight_ref[i * width : (i + 1) * width, :], preferred_element_type=f32)
        total = term if total is None else total + term
    out_ref[...] = total.astype(bf16)


def attention_kernel(tokens, blocks, chained, final, *refs):
    query_pos_ref, q_ref = refs[:2]
    refs = refs[2:]
    if tokens is None:
        pos_ref, refs = refs[0], refs[1:]
    block_refs, refs = refs[:blocks], refs[blocks:]
    state, refs = (refs[:3], refs[3:]) if chained else (None, refs)
    outs, (kv, va, bias) = refs[:-3], refs[-3:]
    row = 0
    for block_ref in block_refs:
        n = block_ref.shape[0]
        if tokens is None:
            kv[row : row + n, :] = block_ref[...]
            row += n
            continue
        for first in range(0, n, tokens + 8):
            kv[row : row + tokens, :] = block_ref[first : first + tokens, :]
            tail = block_ref[first + tokens : first + tokens + 8, :tokens].astype(f32)
            pos = tail[0:1, :] * 128.0 + tail[1:2, :]
            bias[:, row : row + tokens] = jnp.where(pos <= query_pos_ref[:, :tokens], 0.0, masked_score)
            row += tokens
    count = kv.shape[0]
    if tokens is None:
        bias[...] = jnp.where(pos_ref[...] <= query_pos_ref[:, :1], 0.0, masked_score)
    va[:, HEAD_DIM:] = jnp.ones((count, HEAD_DIM), bf16)
    heads = kv.shape[1] // (2 * HEAD_DIM)
    factor = math.log2(math.e) / math.sqrt(HEAD_DIM)
    for h in range(heads):
        keys = kv[:, h * HEAD_DIM : (h + 1) * HEAD_DIM]
        va[:, :HEAD_DIM] = kv[:, (heads + h) * HEAD_DIM : (heads + h + 1) * HEAD_DIM]
        for g in range(GROUP):
            columns = slice((h * GROUP + g) * HEAD_DIM, (h * GROUP + g + 1) * HEAD_DIM)
            scores = lax.dot_general(
                q_ref[:, columns], keys, (((1,), (1,)), ((), ())), preferred_element_type=f32
            )
            scores = scores * factor + bias[...]
            top = jnp.max(scores, axis=1, keepdims=True)
            if chained:
                wide = jnp.maximum(top, state[1][:, columns])
                copies = -(-count // HEAD_DIM)
                tops = jnp.concatenate([wide] * copies, axis=1)[:, :count] if copies > 1 else wide[:, :count]
                weights = jnp.exp2(scores - tops)
            else:
                wide = jnp.broadcast_to(top, (top.shape[0], HEAD_DIM))
                weights = jnp.exp2(scores - top)
            part = jnp.dot(weights.astype(bf16), va[...], preferred_element_type=f32)
            numer, denom = part[:, :HEAD_DIM], part[:, HEAD_DIM:]
            if chained:
                scale = jnp.exp2(state[1][:, columns] - wide)
                numer = numer + state[0][:, columns] * scale
                denom = denom + state[2][:, columns] * scale
            if final:
                outs[0][:, columns] = (numer / denom).astype(bf16)
            else:
                outs[0][:, columns] = numer
                outs[1][:, columns] = wide
                outs[2][:, columns] = denom


def unpack_kernel(source_ref, out_ref):
    half = out_ref.shape[2]
    out_ref[:, 0, :] = source_ref[:, :half]
    out_ref[:, 1, :] = source_ref[:, half:]


def hold(value):
    spec = pl.BlockSpec(memory_space=pl.ANY)
    return pl.pallas_call(
        lambda source, target: None,
        out_shape=jax.ShapeDtypeStruct(value.shape, value.dtype),
        in_specs=[spec],
        out_specs=spec,
        input_output_aliases={0: 0},
        compiler_params=pltpu.CompilerParams(vmem_limit_bytes=1 << 20),
        name="hold",
    )(value)


def join_kernel(*refs):
    row = 0
    for ref in refs[:-1]:
        refs[-1][row : row + ref.shape[0], :] = ref[...]
        row += ref.shape[0]


def join(blocks):
    rows = sum(block.shape[0] for block in blocks)
    return vmem_call(
        join_kernel,
        jax.ShapeDtypeStruct((rows, blocks[0].shape[1]), blocks[0].dtype),
        flops=1 << 16,
        nbytes=4 * rows * blocks[0].shape[1],
    )(*blocks)


def attend(query_pos, queries, pos, blocks, state, tokens, final):
    rows, width = queries.shape
    if tokens is None:
        count = sum(block.shape[0] for block in blocks)
        head_args = (query_pos, queries, pos)
    else:
        count = sum(block.shape[0] // (tokens + 8) * tokens for block in blocks)
        head_args = (query_pos, queries)
    wide = jax.ShapeDtypeStruct((rows, width), f32)
    return vmem_call(
        functools.partial(attention_kernel, tokens, len(blocks), state is not None, final),
        jax.ShapeDtypeStruct((rows, width), bf16) if final else (wide, wide, wide),
        scratch=(
            pltpu.VMEM((count, blocks[0].shape[1]), bf16),
            pltpu.VMEM((count, 2 * HEAD_DIM), bf16),
            pltpu.VMEM((rows, count), f32),
        ),
        flops=4 * rows * width * count,
        nbytes=2 * queries.size + 2 * count * blocks[0].shape[1],
        trans=rows * width // HEAD_DIM * count,
        keep=not final,
    )(*head_args, *blocks, *(state or ()))


def per_device(
    patches,
    ln_gain,
    ln_bias,
    qkv_weight,
    proj_weight,
    proj_bias,
    merge_gain,
    merge_bias,
    visual_kv_weight,
    image_tokens,
    text_before,
    text_order,
    queries,
    text_kv,
):
    seq_count = lax.axis_size("seq")
    head_count = lax.axis_size("head")
    patch_rows, model_width = patches.shape
    merged_rows = patch_rows // 4
    head_cols = qkv_weight.shape[2]
    tokens = queries.shape[0]
    kv_width = text_kv.shape[1] * text_kv.shape[2]
    small = is_small(seq_count, head_count)
    near_count = 3 * patch_rows
    share = jax.ShapeDtypeStruct

    ahead = [(2 * i, 2 * i + 2) for i in range(seq_count - 1)]
    back = [(2 * i + 3, 2 * i + 1) for i in range(seq_count - 1)]
    near_first = lax.ppermute(patches, ("seq", "head"), ahead + back)

    block, query_pos, vit_bias, vis_pos = vmem_call(
        functools.partial(prep_kernel, (seq_count, small, patch_rows, merged_rows)),
        (
            share((tokens + 8, kv_width), bf16),
            share((tokens, LANES), f32),
            share((patch_rows, near_count), f32),
            share((1, merged_rows * seq_count), f32),
        ),
        scratch=(
            pltpu.SMEM(image_tokens.shape, jnp.int32),
            pltpu.SMEM(text_before.shape, jnp.int32),
            pltpu.VMEM((1, tokens), jnp.int32),
            pltpu.VMEM(text_kv.shape, bf16),
            pltpu.SemaphoreType.DMA((4,)),
        ),
        spaces={i: pltpu.HBM for i in range(4)},
        flops=1 << 20,
        nbytes=1 << 20,
    )(image_tokens, text_before, text_order[None, :], text_kv)
    pair_swap = [(i, i ^ 1) for i in range(seq_count)]
    jumps = [[(i, i ^ (2 * k)) for i in range(seq_count)] for k in range(1, seq_count // 2)]
    if small:
        column = [block]
        for jump in jumps:
            column.append(lax.ppermute(block, "seq", jump))
        column.append(lax.ppermute(block, "seq", pair_swap))
        pieces = join(column[1:4])
        column.append(lax.ppermute(pieces, "seq", pair_swap))
        text_blocks = [column]
    else:
        gathered = lax.all_gather(block, "seq", axis=0, tiled=True)
        step = 8 * (tokens + 8)
        text_blocks = [[gathered[i : i + step]] for i in range(0, gathered.shape[0], step)]

    weight = jnp.transpose(qkv_weight, (1, 0, 2))
    cols = share((patch_rows, head_cols), bf16)
    carried = [patches, ln_gain, ln_bias, proj_bias, merge_gain, merge_bias]
    query, key_own, value_own, weight_kv, *carried = vmem_call(
        functools.partial(own_kernel, len(carried)),
        (cols, cols, cols, share((2, model_width, head_cols), bf16), *[share(a.shape, a.dtype) for a in carried]),
        scratch=(pltpu.VMEM((model_width, head_cols), bf16), pltpu.SemaphoreType.DMA((3 + len(carried),))),
        spaces={i: pltpu.HBM for i in range(1 + len(carried))},
        flops=2 * patch_rows * weight.size,
        nbytes=2 * weight.size,
    )(weight, *carried)
    patches, ln_gain, ln_bias, proj_bias, merge_gain, merge_bias = carried

    key_near, value_near = vmem_call(
        near_kernel, (cols, cols), flops=4 * patch_rows * model_width * head_cols, nbytes=2 * weight_kv.size
    )(ln_gain, ln_bias, weight_kv, near_first)
    head_swap = [(0, 1), (1, 0)]
    near_second = lax.ppermute(near_first, "head", head_swap)
    mine_part = vmem_call(
        functools.partial(vit_kernel, 2),
        share((patch_rows, model_width), bf16),
        scratch=(
            pltpu.VMEM((near_count, head_cols), bf16),
            pltpu.VMEM((near_count, head_cols), bf16),
            pltpu.VMEM((patch_rows, head_cols), bf16),
        ),
        flops=4 * patch_rows * near_count * head_cols + 2 * patch_rows * head_cols * model_width,
        nbytes=2 * proj_weight.size,
        trans=patch_rows * near_count * head_cols // VIT_HD,
    )(ln_gain, ln_bias, weight_kv, vit_bias, proj_weight, query, key_own, key_near, value_own, value_near, near_second)
    other_part = lax.ppermute(mine_part, "head", head_swap)
    map_weight = hold(visual_kv_weight.reshape(4 * model_width, -1))
    visual = vmem_call(
        merge_kernel,
        share((merged_rows, kv_width), bf16),
        scratch=(pltpu.VMEM((patch_rows * (model_width // LANES), LANES), f32),),
        flops=2 * merged_rows * map_weight.size,
        nbytes=2 * map_weight.size,
    )(patches, mine_part, other_part, proj_bias, merge_gain, merge_bias, map_weight)

    if small:
        visual_blocks = [[visual]]
        for k in SHIFTS:
            visual_blocks[0].append(lax.ppermute(visual, "seq", [(i, i ^ k) for i in range(seq_count)]))
    else:
        gathered = lax.all_gather(visual, "seq", axis=0, tiled=True)
        step = 8 * merged_rows
        visual_blocks = [[gathered[i : i + step]] for i in range(0, gathered.shape[0], step)]

    visual_out = vmem_call(unpack_kernel, share((merged_rows,) + text_kv.shape[1:], bf16), flops=1 << 16)(visual)
    state = None
    for text_block in text_blocks:
        state = attend(query_pos, queries, None, text_block, state, tokens, False)
    first = 0
    for i, visual_block in enumerate(visual_blocks):
        count = sum(b.shape[0] for b in visual_block)
        final = i == len(visual_blocks) - 1
        pos = vis_pos[:, first : first + count]
        state = attend(query_pos, queries, pos, visual_block, state, None, final)
        first += count
    return (state, visual_out)


def is_small(seq_count, head_count):
    return seq_count == 8 and head_count == 2


def solution(mesh):
    in_specs = (
        P(("grp", "seq"), None),
        P(),
        P(),
        P(None, None, "head"),
        P("head", None),
        P(),
        P(),
        P(),
        P(None, None, "head"),
        P("grp"),
        P("grp"),
        P(("grp", "seq")),
        P(("grp", "seq"), "head"),
        P(("grp", "seq"), None, "head"),
    )
    out_specs = (P(("grp", "seq"), "head"), P(("grp", "seq"), None, "head"))

    return jax.shard_map(per_device, mesh=mesh, in_specs=in_specs, out_specs=out_specs, check_vma=False)
```
